128 devices in a mesh: row: 8 (over y_hi, x), col: 16 (over z, y_lo, core).
Axes of the slice: x: 4, y: 4 (y_hi: 2, y_lo: 2; y = y_hi * 2 + y_lo), z: 4, core: 2. Of those that a mesh axis runs over, the one named last changes fastest.
Arguments:
- integrals: bfloat16 [2400, 2400, 256], P('row', 'col'), may hold values from -6 to 6
- occ_coef: bfloat16 [2400, 96], P('row'), may hold values from -0.125 to 0.125
- virt_coef: bfloat16 [2400, 2304], P('col'), may hold values from -0.125 to 0.125
- pair_index: int32 [256], replicated, may hold values from 0 to 255, each once
Outputs:
- transformed: bfloat16 [96, 2304, 256], P('row', 'col')
The draws below stay inside these ranges and needn't reach their ends.
Inputs may be any that keep to these rules, and one draw needn't show every extreme that they name: pair_index holds each of 0 to 255 once.
All inputs are finite; a program needn't handle non-finite values.
Results may differ from the reference program's by a relative error of at most 0.0049.
Values may be sent and summed in bfloat16 or wider, within the bound.
A program may use at most 192 MiB of HBM per device.

```python
import jax
import jax.numpy as jnp
from jax import lax

O = 96
V = 2304
N = 2400
P_SIZE = 256


def block_scale(stream_key, shape, pieces, low, top_value):
    level = 1.0
    for position, blocks in pieces:
        heights = jax.random.uniform(jax.random.fold_in(jax.random.fold_in(stream_key, 6), position), (blocks,), jnp.float32, low / len(pieces), top_value / len(pieces))
        level = level * jnp.repeat(jnp.exp(heights), shape[position] // blocks).reshape((-1,) + (1,) * (len(shape) - 1 - position))
    return level


def centred(rng, shape, deviation, reach, shards=(), dtype=jnp.bfloat16):
    level = block_scale(rng, shape, shards, -0.22, 0.18) if shards else 1.0
    drawn = jax.random.normal(rng, shape, jnp.float32) * deviation * level
    return jnp.minimum(jnp.maximum(drawn, -reach), reach).astype(dtype)


def setup_inputs(seed: int = 0) -> dict:
    arg_keys = jax.random.split(jax.random.key(seed), 5)
    integrals = centred(arg_keys[0], (N, N, P_SIZE), 1.0, 6.0, ((0, 8), (1, 16)))
    occ_coef = centred(arg_keys[1], (N, O), N ** -0.5, 0.125, ((0, 8),))
    virt_coef = centred(arg_keys[2], (N, V), N ** -0.5, 0.125, ((0, 16),))
    pair_index = jax.random.permutation(arg_keys[3], P_SIZE).astype(jnp.int32)
    return {"integrals": integrals, "occ_coef": occ_coef, "virt_coef": virt_coef, "pair_index": pair_index}


def reference(integrals, occ_coef, virt_coef, pair_index):
    def one_pair(pair_block):
        half_rows = jnp.dot(occ_coef.T, pair_block, preferred_element_type=jnp.float32).astype(jnp.bfloat16)
        return jnp.dot(half_rows, virt_coef, preferred_element_type=jnp.float32).astype(jnp.bfloat16)

    slab_rows = lax.map(one_pair, jnp.moveaxis(integrals, 2, 0))
    chosen = jnp.take(slab_rows, pair_index.astype(jnp.int32), axis=0)
    return jnp.moveaxis(chosen, 0, 2)
```

```python
import functools

import jax
import jax.numpy as jnp
from jax import lax
from jax.experimental import pallas as pl
from jax.experimental.pallas import tpu as pltpu
from jax.sharding import PartitionSpec as P

MESH = pl.DeviceIdType.MESH
BF = jnp.bfloat16
F32 = jnp.float32

N_MU = 300
N_NU = 150
O_LOC = 12
A_LOC = 144
NP = 256
TILES = 19
CHUNKS = (4, 4, 4, 4, 3)
STARTS = tuple(sum(CHUNKS[:k]) for k in range(len(CHUNKS)))
BLK = O_LOC * 8
KROWS = N_MU * 8
NBUF = 3

(X1P, X1M, RAWP, RAWM, ACCP, ACCM, YH, AZP, AZM, AY, AC, BZP, BZM, BC, CZP, CZM, CCP, CCM, DC) = range(19)
NSEM = 19

ORDER = (
    ("M", 0), ("X", 0), ("M", 1), ("S", 0), ("X", 1), ("V", 0), ("Y", 0), ("M", 2), ("S", 1), ("X", 2),
    ("H", 0), ("Y", 1), ("B", 0), ("M", 3), ("S", 2), ("X", 3), ("C", 0), ("H", 1), ("B", 1), ("Y", 2),
    ("M", 4), ("S", 3), ("X", 4), ("D", 0), ("E", 0), ("C", 1), ("H", 2), ("B", 2), ("Y", 3), ("S", 4),
    ("D", 1), ("E", 1), ("C", 2), ("H", 3), ("B", 3), ("Y", 4), ("D", 2), ("E", 2), ("H", 4), ("B", 4), ("C", 3),
    ("D", 3), ("E", 3), ("C", 4), ("D", 4), ("E", 4),
)


def kernel(
    ints, occ_rep, virt, onehot, out,
    ibuf, kron, expand, part, r1p, r1m, r2p, r2m, ry, gath, vrecv, vrows, vt, acc,
    isem, vsend, vrecv_sem, send, recv,
):
    row = lax.axis_index("row")
    col = lax.axis_index("col")
    yh, x = row // 4, row % 4
    z, yl, core = col // 4, (col // 2) % 2, col % 2
    xp, xm = (x + 1) % 4, (x + 3) % 4
    x2 = (x + 2) % 4
    zp, zm, z2 = (z + 1) % 4, (z + 3) % 4, (z + 2) % 4

    def rowid(xx, yy):
        return {"row": yy * 4 + xx}

    def colid(zz, ll, cc):
        return {"col": zz * 4 + ll * 2 + cc}

    d_xp, d_xm, d_yh = rowid(xp, yh), rowid(xm, yh), rowid(x, 1 - yh)
    d_zp, d_zm = colid(zp, yl, core), colid(zm, yl, core)
    d_yl, d_co = colid(z, 1 - yl, core), colid(z, yl, 1 - core)

    def slot(zz, ll, cc):
        return cc * 8 + zz * 2 + ll

    me = slot(z, yl, core)

    barrier = pltpu.get_barrier_semaphore()
    for d in (d_xp, d_xm, d_yh):
        pl.semaphore_signal(barrier, inc=1, device_id=d, device_id_type=MESH)

    @pl.loop(1, 16)
    def _(k):
        pl.semaphore_signal(barrier, inc=1, device_id={"col": (col + k) % 16}, device_id_type=MESH)

    def icopy(t, s):
        return pltpu.make_async_copy(ints.at[:, pl.ds(pl.multiple_of(t * 8, 8), 8), :], ibuf.at[s], isem.at[s])

    def icopy_last(s):
        return pltpu.make_async_copy(
            ints.at[:, pl.ds(8 * (TILES - 1), 6), :], ibuf.at[s, :, pl.ds(0, 6), :], isem.at[s]
        )

    for t in range(NBUF):
        icopy(t, t).start()

    expand[...] = jnp.where(
        lax.broadcasted_iota(jnp.int32, (N_MU, KROWS), 0) == lax.broadcasted_iota(jnp.int32, (N_MU, KROWS), 1) // 8,
        1.0, 0.0,
    ).astype(BF)

    @pl.loop(0, 8)
    def _(b):
        rows = pl.ds(pl.multiple_of(b * BLK, BLK), BLK)
        wide = jnp.dot(occ_rep[rows, :], expand[...], preferred_element_type=F32)
        same = (
            lax.broadcasted_iota(jnp.int32, (BLK, KROWS), 0) % 8 == lax.broadcasted_iota(jnp.int32, (BLK, KROWS), 1) % 8
        )
        kron[rows, :] = jnp.where(same, wide, 0.0).astype(BF)

    pl.semaphore_wait(barrier, 18)

    sent = []

    def remote(src, dst, c, k, dev):
        cp = pltpu.make_async_remote_copy(
            src_ref=src, dst_ref=dst, send_sem=send.at[c * NSEM + k], recv_sem=recv.at[c * NSEM + k],
            device_id=dev, device_id_type=MESH,
        )
        return cp

    cps = {}

    def go(c, k, src, dst, dev):
        cp = remote(src, dst, c, k, dev)
        cp.start()
        cps[c, k] = cp
        sent.append(cp)

    def vcopy(k):
        to = (col + k) % 16
        to_slot = slot(to // 4, (to // 2) % 2, to % 2)
        return pltpu.make_async_remote_copy(
            src_ref=virt.at[to_slot], dst_ref=vrecv.at[me], send_sem=vsend.at[k], recv_sem=vrecv_sem.at[k],
            device_id={"col": to}, device_id_type=MESH,
        )

    def vlocal():
        return pltpu.make_async_copy(virt.at[me], vrecv.at[me], vsend.at[0])

    vlocal().start()

    @pl.loop(1, 16)
    def _(k):
        vcopy(k).start()

    def tiles(c):
        return pl.ds(STARTS[c], CHUNKS[c])

    def blk(xx, yy):
        return pl.ds(pl.multiple_of(xx * (2 * BLK) + yy * BLK, BLK), BLK)

    def task_m(c):
        @pl.loop(STARTS[c], STARTS[c] + CHUNKS[c])
        def _(t):
            s = t % NBUF

            @pl.when(t < TILES - 1)
            def _():
                icopy(t, s).wait()

            @pl.when(t == TILES - 1)
            def _():
                icopy_last(s).wait()

            rhs = ibuf[s].reshape(KROWS, NP)
            part[t] = jnp.dot(kron[...], rhs, preferred_element_type=F32).astype(BF)

            @pl.when(t + NBUF < TILES - 1)
            def _():
                icopy(t + NBUF, s).start()

            @pl.when(t + NBUF == TILES - 1)
            def _():
                icopy_last(s).start()

    def task_x(c):
        ts = tiles(c)
        go(c, X1P, part.at[ts, blk(x2, 0)], r1p.at[ts], d_xp)
        go(c, X1M, part.at[ts, blk(x2, 1)], r1m.at[ts], d_xm)
        go(c, RAWP, part.at[ts, blk(xp, 1)], r2p.at[ts, pl.ds(BLK, BLK)], d_xp)
        go(c, RAWM, part.at[ts, blk(xm, 0)], r2m.at[ts, pl.ds(0, BLK)], d_xm)

    def each_tile(c, body):
        pl.loop(STARTS[c], STARTS[c] + CHUNKS[c])(body)

    def task_s(c):
        ts = tiles(c)
        cps[c, X1P].wait_recv()

        @functools.partial(each_tile, c)
        def _(t):
            b = blk(xp, 0)
            part[t, b, :] = (part[t, b, :].astype(F32) + r1p[t].astype(F32)).astype(BF)

        go(c, ACCP, part.at[ts, blk(xp, 0)], r2p.at[ts, pl.ds(0, BLK)], d_xp)
        cps[c, X1M].wait_recv()

        @functools.partial(each_tile, c)
        def _(t):
            b = blk(xm, 1)
            part[t, b, :] = (part[t, b, :].astype(F32) + r1m[t].astype(F32)).astype(BF)

        go(c, ACCM, part.at[ts, blk(xm, 1)], r2m.at[ts, pl.ds(BLK, BLK)], d_xm)

    def xsum(t, yy):
        side = pl.ds(pl.multiple_of(yy * BLK, BLK), BLK)
        return part[t, blk(x, yy), :].astype(F32) + r2p[t, side, :].astype(F32) + r2m[t, side, :].astype(F32)

    def task_y(c):
        ts = tiles(c)
        for k in (RAWP, RAWM, ACCP, ACCM):
            cps[c, k].wait_recv()

        @functools.partial(each_tile, c)
        def _(t):
            part[t, blk(x, 1 - yh), :] = xsum(t, 1 - yh).astype(BF)

        go(c, YH, part.at[ts, blk(x, 1 - yh)], ry.at[ts], d_yh)

    def grows(c, s, count=1):
        n = 8 * CHUNKS[c]
        return pl.ds(pl.multiple_of(128 * STARTS[c] + s * n, 8), count * n)

    def whole(c, s, count=1):
        return gath.at[:, grows(c, s, count), :]

    def half(c, s, lo):
        return gath.at[pl.ds(lo, O_LOC // 2), grows(c, s, 2), :]

    def task_h(c):
        cps[c, YH].wait_recv()
        base = 128 * STARTS[c] + me * (8 * CHUNKS[c])

        @functools.partial(each_tile, c)
        def _(t):
            h = (xsum(t, yh) + ry[t].astype(F32)).astype(BF)
            h = jnp.dot(h, onehot[...], preferred_element_type=F32).astype(BF)
            dst = pl.ds(pl.multiple_of(base + (t - STARTS[c]) * 8, 8), 8)
            gath[:, dst, :] = h.reshape(O_LOC, 8, NP)

        g = whole(c, me)
        go(c, AY, g, g, d_yl)
        go(c, AZP, g, g, d_zp)
        go(c, AZM, g, g, d_zm)
        go(c, AC, g, g, d_co)

    def task_b(c):
        cps[c, AY].wait_recv()
        g = whole(c, slot(z, 1 - yl, core))
        go(c, BZP, g, g, d_zp)
        go(c, BZM, g, g, d_zm)
        go(c, BC, g, g, d_co)

    def task_c(c):
        cps[c, AZP].wait_recv()
        cps[c, BZP].wait_recv()
        s = slot(zm, 0, core)
        g = half(c, s, 0)
        go(c, CZP, g, g, d_zp)
        g = whole(c, s, 2)
        go(c, CCP, g, g, d_co)
        cps[c, AZM].wait_recv()
        cps[c, BZM].wait_recv()
        s = slot(zp, 0, core)
        g = half(c, s, O_LOC // 2)
        go(c, CZM, g, g, d_zm)
        g = whole(c, s, 2)
        go(c, CCM, g, g, d_co)

    def task_d(c):
        cps[c, CZP].wait_recv()
        cps[c, CZM].wait_recv()
        g = whole(c, slot(z2, 0, core), 2)
        go(c, DC, g, g, d_co)

    def task_v(_):
        vlocal().wait()

        @pl.loop(1, 16)
        def _(k):
            vcopy(k).wait()

        for c in range(len(CHUNKS)):
            n = 8 * CHUNKS[c]

            @pl.loop(0, 16)
            def _(s):
                dst = pl.ds(pl.multiple_of(128 * STARTS[c] + s * n, 8), n)
                vrows[dst, :] = vrecv[s, pl.ds(8 * STARTS[c], n), :]

        @pl.loop(0, TILES)
        def _(t):
            o = pl.multiple_of(t * 128, 128)
            vt[:, pl.ds(o, 128)] = vrows[pl.ds(o, 128), :].astype(F32).T[:A_LOC].astype(BF)

    def task_e(c):
        for k in (AC, BC, CCP, CCM, DC):
            cps[c, k].wait_recv()
        ks = pl.ds(128 * STARTS[c], 128 * CHUNKS[c])
        lhs = vt[:, ks]
        last = c == len(CHUNKS) - 1

        @pl.loop(0, O_LOC)
        def _(i):
            d = jnp.dot(lhs, gath[i, ks, :], preferred_element_type=F32)
            if c > 0:
                d = d + acc[i]
            if last:
                out[i] = d.astype(BF)
            else:
                acc[i] = d

    tasks = {"M": task_m, "X": task_x, "S": task_s, "Y": task_y, "H": task_h, "B": task_b, "C": task_c,
             "D": task_d, "E": task_e, "V": task_v}
    for name, c in ORDER:
        tasks[name](c)
    for cp in sent:
        cp.wait_send()


def local(integrals, occ_coef, virt_coef, pair_index):
    occ = occ_coef.T.reshape(2, 4, O_LOC, N_MU).transpose(1, 0, 2, 3).reshape(8 * O_LOC, N_MU)
    occ_rep = jnp.repeat(occ, 8, axis=0)
    virt = virt_coef.reshape(N_NU, 4, 2, 2, A_LOC).transpose(3, 1, 2, 0, 4).reshape(16, N_NU, A_LOC)
    virt = jnp.pad(virt, ((0, 0), (0, 8 * TILES - N_NU), (0, NP - A_LOC)))
    onehot = (jnp.arange(NP, dtype=jnp.int32)[:, None] == pair_index[None, :]).astype(BF)
    nsem = NSEM * len(CHUNKS)
    vm = pl.BlockSpec(memory_space=pltpu.VMEM)
    hbm = pl.BlockSpec(memory_space=pl.ANY)
    return pl.pallas_call(
        kernel,
        out_shape=jax.ShapeDtypeStruct((O_LOC, A_LOC, NP), BF),
        in_specs=[hbm, vm, hbm, vm],
        out_specs=vm,
        scratch_shapes=[
            pltpu.VMEM((NBUF, N_MU, 8, NP), BF),
            pltpu.VMEM((8 * BLK, KROWS), BF),
            pltpu.VMEM((N_MU, KROWS), BF),
            pltpu.VMEM((TILES, 8 * BLK, NP), BF),
            pltpu.VMEM((TILES, BLK, NP), BF),
            pltpu.VMEM((TILES, BLK, NP), BF),
            pltpu.VMEM((TILES, 2 * BLK, NP), BF),
            pltpu.VMEM((TILES, 2 * BLK, NP), BF),
            pltpu.VMEM((TILES, BLK, NP), BF),
            pltpu.VMEM((O_LOC, TILES * 128, NP), BF),
            pltpu.VMEM((16, 8 * TILES, NP), BF),
            pltpu.VMEM((TILES * 128, NP), BF),
            pltpu.VMEM((A_LOC, TILES * 128), BF),
            pltpu.VMEM((O_LOC, A_LOC, NP), F32),
            pltpu.SemaphoreType.DMA((NBUF,)),
            pltpu.SemaphoreType.DMA((16,)),
            pltpu.SemaphoreType.DMA((16,)),
            pltpu.SemaphoreType.DMA((nsem,)),
            pltpu.SemaphoreType.DMA((nsem,)),
        ],
        compiler_params=pltpu.CompilerParams(
            collective_id=0, has_side_effects=True, vmem_limit_bytes=60 * 2**20
        ),
    )(integrals, occ_rep, virt, onehot)


def solution(mesh):
    return jax.shard_map(
        local,
        mesh=mesh,
        in_specs=(P("row", "col", None), P("row", None), P("col", None), P()),
        out_specs=P("row", "col", None),
        check_vma=False,
    )
```

```python
import functools

import jax
import jax.numpy as jnp
from jax import lax
from jax.experimental import pallas as pl
from jax.experimental.pallas import tpu as pltpu
from jax.sharding import PartitionSpec as P

MESH = pl.DeviceIdType.MESH
BF = jnp.bfloat16
F32 = jnp.float32

N_MU = 300
N_NU = 150
O_LOC = 12
A_LOC = 144
NP = 256
TILES = 19
CHUNKS = (2, 2, 3, 2, 3, 2, 2, 3)
STARTS = tuple(sum(CHUNKS[:k]) for k in range(len(CHUNKS)))
BLK = O_LOC * 8
KROWS = N_MU * 8
NBUF = 3

(X1P, X1M, RAWP, RAWM, ACCP, ACCM, YH, AZP, AZM, AY, AC, BZP, BZM, BC, CZP, CZM, CCP, CCM, DC) = range(19)
NSEM = 19

ORDER = (
    ("VS", 0), ("VP", 0), ("M", 0, 0, 2), ("X", 0), ("M", 1, 0, 2), ("X", 1), ("SM", 0), ("SP", 0), ("M", 2, 0, 2),
    ("SM", 1), ("SP", 1), ("M", 2, 2, 1), ("M", 3, 0, 2), ("X", 2), ("Y", 0), ("Y", 1), ("M", 4, 0, 2), ("X", 3),
    ("SM", 2), ("SP", 2), ("H", 0), ("H", 1), ("SM", 3), ("SP", 3), ("B", 0), ("M", 4, 2, 1), ("B", 1),
    ("M", 5, 0, 2), ("X", 4), ("Y", 2), ("CM", 0), ("CP", 0), ("CM", 1), ("CP", 1), ("Y", 3), ("M", 6, 0, 2),
    ("X", 5), ("D", 0), ("SM", 4), ("SP", 4), ("H", 2), ("D", 1), ("H", 3), ("SM", 5), ("SP", 5), ("M", 7, 0, 2),
    ("B", 2), ("M", 7, 2, 1), ("X", 6), ("B", 3), ("Y", 4), ("Y", 5), ("X", 7), ("CM", 2), ("CP", 2), ("SM", 6),
    ("SP", 6), ("CM", 3), ("CP", 3), ("H", 4), ("D", 2), ("H", 5), ("SM", 7), ("SP", 7), ("D", 3), ("VT", 0),
    ("B", 4), ("Y", 6), ("B", 5), ("E", 0), ("Y", 7), ("CM", 4), ("CP", 4), ("H", 6), ("CM", 5), ("CP", 5), ("E", 1),
    ("D", 4), ("H", 7), ("B", 6), ("E", 2), ("D", 5), ("E", 3), ("B", 7), ("E", 4), ("CM", 6), ("CP", 6), ("E", 5),
    ("CM", 7), ("CP", 7), ("D", 6), ("E", 6), ("D", 7), ("E", 7),
)


def kernel(
    ints, occ_t, virt, index, out,
    ibuf, kron, expand, occ_rep, onehot, part, r1p, r1m, r2p, r2m, ry, gath, vraw, vblk, vrecv, vrows, vt, acc,
    isem, vload, vsend, vrecv_sem, send, recv,
):
    row = lax.axis_index("row")
    col = lax.axis_index("col")
    yh, x = row // 4, row % 4
    z, yl, core = col // 4, (col // 2) % 2, col % 2
    xp, xm = (x + 1) % 4, (x + 3) % 4
    x2 = (x + 2) % 4
    zp, zm, z2 = (z + 1) % 4, (z + 3) % 4, (z + 2) % 4

    def rowid(xx, yy):
        return {"row": yy * 4 + xx}

    def colid(zz, ll, cc):
        return {"col": zz * 4 + ll * 2 + cc}

    d_xp, d_xm, d_yh = rowid(xp, yh), rowid(xm, yh), rowid(x, 1 - yh)
    d_zp, d_zm = colid(zp, yl, core), colid(zm, yl, core)
    d_yl, d_co = colid(z, 1 - yl, core), colid(z, yl, 1 - core)

    def slot(zz, ll, cc):
        return cc * 8 + zz * 2 + ll

    me = slot(z, yl, core)

    barrier = pltpu.get_barrier_semaphore()
    for d in (d_xp, d_xm, d_yh):
        pl.semaphore_signal(barrier, inc=1, device_id=d, device_id_type=MESH)

    @pl.loop(1, 16)
    def _(k):
        pl.semaphore_signal(barrier, inc=1, device_id={"col": (col + k) % 16}, device_id_type=MESH)

    def icopy(t, s):
        return pltpu.make_async_copy(ints.at[:, pl.ds(pl.multiple_of(t * 8, 8), 8), :], ibuf.at[s], isem.at[s])

    def icopy_last(s):
        return pltpu.make_async_copy(
            ints.at[:, pl.ds(8 * (TILES - 1), 6), :], ibuf.at[s, :, pl.ds(0, 6), :], isem.at[s]
        )

    for t in range(NBUF):
        icopy(t, t).start()

    def vfetch():
        return pltpu.make_async_copy(virt, vraw, vload)

    vfetch().start()

    def iota(shape, axis):
        return lax.broadcasted_iota(jnp.int32, shape, axis)

    for b in range(8):
        first = ((b % 2) * 4 + b // 2) * O_LOC
        pick = jnp.where(iota((BLK, BLK), 1) == first + (iota((BLK, BLK), 0) >> 3), 1.0, 0.0).astype(BF)
        occ_rep[b * BLK : (b + 1) * BLK, :] = jnp.dot(pick, occ_t[...], preferred_element_type=F32).astype(BF)
    expand[...] = jnp.where(iota((N_MU, KROWS), 0) == (iota((N_MU, KROWS), 1) >> 3), 1.0, 0.0).astype(BF)

    @pl.loop(0, 4)
    def _(b):
        rows = pl.ds(pl.multiple_of(b * (2 * BLK), 2 * BLK), 2 * BLK)
        wide = jnp.dot(occ_rep[rows, :], expand[...], preferred_element_type=F32)
        same = (iota((2 * BLK, KROWS), 0) & 7) == (iota((2 * BLK, KROWS), 1) & 7)
        kron[rows, :] = jnp.where(same, wide, 0.0).astype(BF)

    onehot[...] = jnp.where(iota((NP, NP), 0) == index[...], 1.0, 0.0).astype(BF)

    pl.semaphore_wait(barrier, 18)

    sent = []

    def remote(src, dst, c, k, dev):
        cp = pltpu.make_async_remote_copy(
            src_ref=src, dst_ref=dst, send_sem=send.at[c * NSEM + k], recv_sem=recv.at[c * NSEM + k],
            device_id=dev, device_id_type=MESH,
        )
        return cp

    cps = {}

    def go(c, k, src, dst, dev):
        cp = remote(src, dst, c, k, dev)
        cp.start()
        cps[c, k] = cp
        sent.append(cp)

    def vcopy(k):
        to = (col + k) % 16
        to_slot = slot(to // 4, (to // 2) % 2, to % 2)
        return pltpu.make_async_remote_copy(
            src_ref=vblk.at[to_slot], dst_ref=vrecv.at[me], send_sem=vsend.at[k], recv_sem=vrecv_sem.at[k],
            device_id={"col": to}, device_id_type=MESH,
        )

    def vlocal():
        return pltpu.make_async_copy(vblk.at[me], vrecv.at[me], vsend.at[0])

    def task_vs(_):
        vfetch().wait()
        for k in range(16):
            s = slot(k // 4, (k // 2) % 2, k % 2)
            vblk[s, N_NU - 6 : 8 * TILES, :] = jnp.zeros((8, NP), BF)
            vblk[s, 0:N_NU, 0:A_LOC] = vraw[:, k * A_LOC : (k + 1) * A_LOC]

    def task_vp(_):
        vlocal().start()

        @pl.loop(1, 16)
        def _(k):
            vcopy(k).start()

    def tiles(c):
        return pl.ds(STARTS[c], CHUNKS[c])

    def blk(xx, yy):
        return pl.ds(pl.multiple_of(xx * (2 * BLK) + yy * BLK, BLK), BLK)

    def task_m(c, first, count):
        @pl.loop(STARTS[c] + first, STARTS[c] + first + count)
        def _(t):
            s = t % NBUF

            @pl.when(t < TILES - 1)
            def _():
                icopy(t, s).wait()

            @pl.when(t == TILES - 1)
            def _():
                icopy_last(s).wait()

            rhs = ibuf[s].reshape(KROWS, NP)
            part[t] = jnp.dot(kron[...], rhs, preferred_element_type=F32).astype(BF)

            @pl.when(t + NBUF < TILES - 1)
            def _():
                icopy(t + NBUF, s).start()

            @pl.when(t + NBUF == TILES - 1)
            def _():
                icopy_last(s).start()

    def task_x(c):
        ts = tiles(c)
        go(c, X1P, part.at[ts, blk(x2, 0)], r1p.at[ts], d_xp)
        go(c, X1M, part.at[ts, blk(x2, 1)], r1m.at[ts], d_xm)
        go(c, RAWP, part.at[ts, blk(xp, 1)], r2p.at[ts, pl.ds(BLK, BLK)], d_xp)
        go(c, RAWM, part.at[ts, blk(xm, 0)], r2m.at[ts, pl.ds(0, BLK)], d_xm)

    def each_tile(c, body):
        pl.loop(STARTS[c], STARTS[c] + CHUNKS[c])(body)

    def task_sp(c):
        ts = tiles(c)
        cps[c, X1P].wait_recv()

        @functools.partial(each_tile, c)
        def _(t):
            b = blk(xp, 0)
            part[t, b, :] = (part[t, b, :].astype(F32) + r1p[t].astype(F32)).astype(BF)

        go(c, ACCP, part.at[ts, blk(xp, 0)], r2p.at[ts, pl.ds(0, BLK)], d_xp)

    def task_sm(c):
        ts = tiles(c)
        cps[c, X1M].wait_recv()

        @functools.partial(each_tile, c)
        def _(t):
            b = blk(xm, 1)
            part[t, b, :] = (part[t, b, :].astype(F32) + r1m[t].astype(F32)).astype(BF)

        go(c, ACCM, part.at[ts, blk(xm, 1)], r2m.at[ts, pl.ds(BLK, BLK)], d_xm)

    def xsum(t, yy):
        side = pl.ds(pl.multiple_of(yy * BLK, BLK), BLK)
        return part[t, blk(x, yy), :].astype(F32) + r2p[t, side, :].astype(F32) + r2m[t, side, :].astype(F32)

    def task_y(c):
        ts = tiles(c)
        for k in (RAWP, RAWM, ACCP, ACCM):
            cps[c, k].wait_recv()

        @functools.partial(each_tile, c)
        def _(t):
            part[t, blk(x, 1 - yh), :] = xsum(t, 1 - yh).astype(BF)

        go(c, YH, part.at[ts, blk(x, 1 - yh)], ry.at[ts], d_yh)

    def grows(c, s, count=1):
        n = 8 * CHUNKS[c]
        return pl.ds(pl.multiple_of(128 * STARTS[c] + s * n, 8), count * n)

    def whole(c, s, count=1):
        return gath.at[:, grows(c, s, count), :]

    def half(c, s, lo):
        return gath.at[pl.ds(lo, O_LOC // 2), grows(c, s, 2), :]

    def task_h(c):
        cps[c, YH].wait_recv()
        base = 128 * STARTS[c] + me * (8 * CHUNKS[c])

        @functools.partial(each_tile, c)
        def _(t):
            h = (xsum(t, yh) + ry[t].astype(F32)).astype(BF)
            h = jnp.dot(h, onehot[...], preferred_element_type=F32).astype(BF)
            dst = pl.ds(pl.multiple_of(base + (t - STARTS[c]) * 8, 8), 8)
            gath[:, dst, :] = h.reshape(O_LOC, 8, NP)

        g = whole(c, me)
        go(c, AY, g, g, d_yl)
        go(c, AZP, g, g, d_zp)
        go(c, AZM, g, g, d_zm)
        go(c, AC, g, g, d_co)

    def task_b(c):
        cps[c, AY].wait_recv()
        g = whole(c, slot(z, 1 - yl, core))
        go(c, BZP, g, g, d_zp)
        go(c, BZM, g, g, d_zm)
        go(c, BC, g, g, d_co)

    def task_cp(c):
        cps[c, AZP].wait_recv()
        cps[c, BZP].wait_recv()
        s = slot(zm, 0, core)
        g = half(c, s, 0)
        go(c, CZP, g, g, d_zp)
        g = whole(c, s, 2)
        go(c, CCP, g, g, d_co)

    def task_cm(c):
        cps[c, AZM].wait_recv()
        cps[c, BZM].wait_recv()
        s = slot(zp, 0, core)
        g = half(c, s, O_LOC // 2)
        go(c, CZM, g, g, d_zm)
        g = whole(c, s, 2)
        go(c, CCM, g, g, d_co)

    def task_d(c):
        cps[c, CZP].wait_recv()
        cps[c, CZM].wait_recv()
        g = whole(c, slot(z2, 0, core), 2)
        go(c, DC, g, g, d_co)

    def task_vt(_):
        vlocal().wait()

        @pl.loop(1, 16)
        def _(k):
            vcopy(k).wait()

        for c in range(len(CHUNKS)):
            n = 8 * CHUNKS[c]

            @pl.loop(0, 16)
            def _(s):
                dst = pl.ds(pl.multiple_of(128 * STARTS[c] + s * n, 8), n)
                vrows[dst, :] = vrecv[s, pl.ds(8 * STARTS[c], n), :]

        @pl.loop(0, TILES)
        def _(t):
            o = pl.multiple_of(t * 128, 128)
            vt[:, pl.ds(o, 128)] = vrows[pl.ds(o, 128), :].astype(F32).T[:A_LOC].astype(BF)

    def task_e(c):
        for k in (AC, BC, CCP, CCM, DC):
            cps[c, k].wait_recv()
        ks = pl.ds(128 * STARTS[c], 128 * CHUNKS[c])
        lhs = vt[:, ks]
        last = c == len(CHUNKS) - 1

        @pl.loop(0, O_LOC)
        def _(i):
            d = jnp.dot(lhs, gath[i, ks, :], preferred_element_type=F32)
            if c > 0:
                d = d + acc[i]
            if last:
                out[i] = d.astype(BF)
            else:
                acc[i] = d

    tasks = {"M": task_m, "X": task_x, "SP": task_sp, "SM": task_sm, "Y": task_y, "H": task_h, "B": task_b,
             "CP": task_cp, "CM": task_cm, "D": task_d, "E": task_e, "VS": task_vs, "VP": task_vp, "VT": task_vt}
    for name, *where in ORDER:
        tasks[name](*where)
    for cp in sent:
        cp.wait_send()


def local(integrals, occ_coef, virt_coef, pair_index):
    nsem = NSEM * len(CHUNKS)
    vm = pl.BlockSpec(memory_space=pltpu.VMEM)
    hbm = pl.BlockSpec(memory_space=pl.ANY)
    return pl.pallas_call(
        kernel,
        out_shape=jax.ShapeDtypeStruct((O_LOC, A_LOC, NP), BF),
        in_specs=[hbm, vm, hbm, vm],
        out_specs=vm,
        scratch_shapes=[
            pltpu.VMEM((NBUF, N_MU, 8, NP), BF),
            pltpu.VMEM((8 * BLK, KROWS), BF),
            pltpu.VMEM((N_MU, KROWS), BF),
            pltpu.VMEM((8 * BLK, N_MU), BF),
            pltpu.VMEM((NP, NP), BF),
            pltpu.VMEM((TILES, 8 * BLK, NP), BF),
            pltpu.VMEM((TILES, BLK, NP), BF),
            pltpu.VMEM((TILES, BLK, NP), BF),
            pltpu.VMEM((TILES, 2 * BLK, NP), BF),
            pltpu.VMEM((TILES, 2 * BLK, NP), BF),
            pltpu.VMEM((TILES, BLK, NP), BF),
            pltpu.VMEM((O_LOC, TILES * 128, NP), BF),
            pltpu.VMEM((N_NU, 16 * A_LOC), BF),
            pltpu.VMEM((16, 8 * TILES, NP), BF),
            pltpu.VMEM((16, 8 * TILES, NP), BF),
            pltpu.VMEM((TILES * 128, NP), BF),
            pltpu.VMEM((A_LOC, TILES * 128), BF),
            pltpu.VMEM((O_LOC, A_LOC, NP), F32),
            pltpu.SemaphoreType.DMA((NBUF,)),
            pltpu.SemaphoreType.DMA,
            pltpu.SemaphoreType.DMA((16,)),
            pltpu.SemaphoreType.DMA((16,)),
            pltpu.SemaphoreType.DMA((nsem,)),
            pltpu.SemaphoreType.DMA((nsem,)),
        ],
        compiler_params=pltpu.CompilerParams(
            collective_id=0, has_side_effects=True, vmem_limit_bytes=60 * 2**20
        ),
    )(integrals, occ_coef.T, virt_coef, pair_index[None, :])


def solution(mesh):
    return jax.shard_map(
        local,
        mesh=mesh,
        in_specs=(P("row", "col", None), P("row", None), P("col", None), P()),
        out_specs=P("row", "col", None),
        check_vma=False,
    )
```

```python
import functools

import jax
import jax.numpy as jnp
from jax import lax
from jax.experimental import pallas as pl
from jax.experimental.pallas import tpu as pltpu
from jax.sharding import PartitionSpec as P

MESH = pl.DeviceIdType.MESH
BF = jnp.bfloat16
F32 = jnp.float32

N_MU = 300
N_NU = 150
O_LOC = 12
A_LOC = 144
NP = 256
TILES = 19
CHUNKS = (2, 2, 3, 2, 2, 3, 3, 2)
Z_FIRST = (6,)
STARTS = tuple(sum(CHUNKS[:k]) for k in range(len(CHUNKS)))
BLK = O_LOC * 8
KROWS = N_MU * 8
NBUF = 3

(X1P, X1M, RAWP, RAWM, ACCP, ACCM, YH, AZP, AZM, AY, AC, BZP, BZM, BC, CZP, CZM, CCP, CCM, DC,
 BYP, BYM, BY2, YCP, YCM, YC2) = range(25)
NSEM = 25

ORDER = (
    ("M", 0, 0, 2), ("X", 0), ("VS", 0), ("VP", 0), ("M", 1, 0, 2), ("X", 1), ("SP", 0), ("M", 2, 0, 2), ("SM", 0),
    ("M", 2, 2, 1), ("SP", 1), ("SM", 1), ("X", 2), ("M", 3, 0, 2), ("M", 4, 0, 2), ("Y", 0), ("X", 3), ("Y", 1),
    ("M", 5, 0, 2), ("SM", 2), ("SP", 2), ("H", 0), ("H", 1), ("SP", 3), ("SM", 3), ("X", 4), ("M", 5, 2, 1),
    ("B", 0), ("M", 6, 0, 2), ("Y", 2), ("B", 1), ("Y", 3), ("X", 5), ("CM", 0), ("CP", 0), ("SM", 4), ("M", 6, 2, 1),
    ("CM", 1), ("CP", 1), ("H", 2), ("H", 3), ("SM", 5), ("SP", 4), ("SP", 5), ("M", 7, 0, 2), ("D", 0), ("B", 2),
    ("X", 6), ("Y", 4), ("B", 3), ("Y", 5), ("CM", 2), ("CP", 2), ("H", 4), ("SM", 6), ("SP", 6), ("CP", 3), ("D", 1),
    ("CM", 3), ("X", 7), ("H", 5), ("B", 4), ("D", 2), ("VT", 0), ("Y", 6), ("SM", 7), ("SP", 7), ("D", 3), ("B", 5),
    ("CM", 4), ("CP", 4), ("Y", 7), ("E", 0), ("H", 6), ("CM", 5), ("CP", 5), ("H", 7), ("D", 4), ("E", 1), ("CP", 6),
    ("CM", 6), ("E", 2), ("E", 3), ("B", 7), ("D", 6), ("CM", 7), ("CP", 7), ("YM", 6), ("E", 4), ("D", 5), ("B", 6),
    ("YP", 6), ("E", 5), ("Y2", 6), ("D", 7), ("E", 6), ("E", 7),
)


def kernel(
    ints, occ_t, virt, index, out,
    ibuf, kron, pick, onehot, part, r1p, r1m, r2p, r2m, ry, gath, vraw, vblk, vrecv, vrows, vt, acc,
    isem, vload, vsend, vrecv_sem, send, recv,
):
    row = lax.axis_index("row")
    col = lax.axis_index("col")
    yh, x = row // 4, row % 4
    z, yl, core = col // 4, (col // 2) % 2, col % 2
    xp, xm = (x + 1) % 4, (x + 3) % 4
    x2 = (x + 2) % 4
    zp, zm, z2 = (z + 1) % 4, (z + 3) % 4, (z + 2) % 4

    def rowid(xx, yy):
        return {"row": yy * 4 + xx}

    def colid(zz, ll, cc):
        return {"col": zz * 4 + ll * 2 + cc}

    d_xp, d_xm, d_yh = rowid(xp, yh), rowid(xm, yh), rowid(x, 1 - yh)
    d_zp, d_zm = colid(zp, yl, core), colid(zm, yl, core)
    d_yl, d_co = colid(z, 1 - yl, core), colid(z, yl, 1 - core)

    def slot(zz, ll, cc):
        return cc * 8 + zz * 2 + ll

    me = slot(z, yl, core)

    barrier = pltpu.get_barrier_semaphore()
    for d in (d_xp, d_xm, d_yh):
        pl.semaphore_signal(barrier, inc=1, device_id=d, device_id_type=MESH)

    @pl.loop(1, 16)
    def _(k):
        pl.semaphore_signal(barrier, inc=1, device_id={"col": (col + k) % 16}, device_id_type=MESH)

    def icopy(t, s):
        return pltpu.make_async_copy(ints.at[:, pl.ds(pl.multiple_of(t * 8, 8), 8), :], ibuf.at[s], isem.at[s])

    def icopy_last(s):
        return pltpu.make_async_copy(
            ints.at[:, pl.ds(8 * (TILES - 1), 6), :], ibuf.at[s, :, pl.ds(0, 6), :], isem.at[s]
        )

    for t in range(NBUF):
        icopy(t, t).start()

    def vfetch():
        return pltpu.make_async_copy(virt, vraw, vload)

    vfetch().start()

    def iota(shape, axis):
        return lax.broadcasted_iota(jnp.int32, shape, axis)

    for b in range(8):
        first = ((b % 2) * 4 + b // 2) * O_LOC
        mine = iota((BLK, 8 * O_LOC), 1) == first + (iota((BLK, 8 * O_LOC), 0) >> 3)
        pick[b * BLK : (b + 1) * BLK, :] = jnp.where(mine, 1.0, 0.0).astype(BF)
    same = ((iota((8, NP), 0) & 7) == (iota((8, NP), 1) & 7))[None]
    for j in range(0, N_MU, 32):
        n = min(32, N_MU - j)
        stretch = jnp.where(iota((n, 8 * n), 0) == (iota((n, 8 * n), 1) >> 3), 1.0, 0.0).astype(BF)
        wide = jnp.dot(occ_t[:, j : j + n], stretch, preferred_element_type=F32).astype(BF)
        wide = jnp.dot(pick[...], wide, preferred_element_type=F32).reshape(8 * O_LOC, 8, 8 * n)
        wide = jnp.where(same[:, :, : 8 * n], wide, 0.0).astype(BF)
        kron[:, 8 * j : 8 * (j + n)] = wide.reshape(8 * BLK, 8 * n)

    onehot[...] = jnp.where(iota((NP, NP), 0) == index[...], 1.0, 0.0).astype(BF)

    pl.semaphore_wait(barrier, 18)

    sent = []

    def remote(src, dst, c, k, dev):
        cp = pltpu.make_async_remote_copy(
            src_ref=src, dst_ref=dst, send_sem=send.at[c * NSEM + k], recv_sem=recv.at[c * NSEM + k],
            device_id=dev, device_id_type=MESH,
        )
        return cp

    cps = {}

    def go(c, k, src, dst, dev):
        cp = remote(src, dst, c, k, dev)
        cp.start()
        cps[c, k] = cp
        sent.append(cp)

    def vcopy(k):
        to = (col + k) % 16
        to_slot = slot(to // 4, (to // 2) % 2, to % 2)
        return pltpu.make_async_remote_copy(
            src_ref=vblk.at[to_slot], dst_ref=vrecv.at[me], send_sem=vsend.at[k], recv_sem=vrecv_sem.at[k],
            device_id={"col": to}, device_id_type=MESH,
        )

    def vlocal():
        return pltpu.make_async_copy(vblk.at[me], vrecv.at[me], vsend.at[0])

    def task_vs(_):
        vfetch().wait()
        for k in range(16):
            s = slot(k // 4, (k // 2) % 2, k % 2)
            vblk[s, N_NU - 6 : 8 * TILES, :] = jnp.zeros((8, NP), BF)
            vblk[s, 0:N_NU, 0:A_LOC] = vraw[:, k * A_LOC : (k + 1) * A_LOC]

    def task_vp(_):
        vlocal().start()

        @pl.loop(1, 16)
        def _(k):
            vcopy(k).start()

    def tiles(c):
        return pl.ds(STARTS[c], CHUNKS[c])

    def blk(xx, yy):
        return pl.ds(pl.multiple_of(xx * (2 * BLK) + yy * BLK, BLK), BLK)

    def task_m(c, first, count):
        @pl.loop(STARTS[c] + first, STARTS[c] + first + count)
        def _(t):
            s = t % NBUF

            @pl.when(t < TILES - 1)
            def _():
                icopy(t, s).wait()

            @pl.when(t == TILES - 1)
            def _():
                icopy_last(s).wait()

            rhs = ibuf[s].reshape(KROWS, NP)
            part[t] = jnp.dot(kron[...], rhs, preferred_element_type=F32).astype(BF)

            @pl.when(t + NBUF < TILES - 1)
            def _():
                icopy(t + NBUF, s).start()

            @pl.when(t + NBUF == TILES - 1)
            def _():
                icopy_last(s).start()

    def task_x(c):
        ts = tiles(c)
        go(c, X1P, part.at[ts, blk(x2, 0)], r1p.at[ts], d_xp)
        go(c, X1M, part.at[ts, blk(x2, 1)], r1m.at[ts], d_xm)
        go(c, RAWP, part.at[ts, blk(xp, 1)], r2p.at[ts, pl.ds(BLK, BLK)], d_xp)
        go(c, RAWM, part.at[ts, blk(xm, 0)], r2m.at[ts, pl.ds(0, BLK)], d_xm)

    def each_tile(c, body):
        pl.loop(STARTS[c], STARTS[c] + CHUNKS[c])(body)

    def task_sp(c):
        ts = tiles(c)
        cps[c, X1P].wait_recv()

        @functools.partial(each_tile, c)
        def _(t):
            b = blk(xp, 0)
            part[t, b, :] = (part[t, b, :].astype(F32) + r1p[t].astype(F32)).astype(BF)

        go(c, ACCP, part.at[ts, blk(xp, 0)], r2p.at[ts, pl.ds(0, BLK)], d_xp)

    def task_sm(c):
        ts = tiles(c)
        cps[c, X1M].wait_recv()

        @functools.partial(each_tile, c)
        def _(t):
            b = blk(xm, 1)
            part[t, b, :] = (part[t, b, :].astype(F32) + r1m[t].astype(F32)).astype(BF)

        go(c, ACCM, part.at[ts, blk(xm, 1)], r2m.at[ts, pl.ds(BLK, BLK)], d_xm)

    def xsum(t, yy):
        side = pl.ds(pl.multiple_of(yy * BLK, BLK), BLK)
        return part[t, blk(x, yy), :].astype(F32) + r2p[t, side, :].astype(F32) + r2m[t, side, :].astype(F32)

    def task_y(c):
        ts = tiles(c)
        for k in (RAWP, RAWM, ACCP, ACCM):
            cps[c, k].wait_recv()

        @functools.partial(each_tile, c)
        def _(t):
            part[t, blk(x, 1 - yh), :] = xsum(t, 1 - yh).astype(BF)

        go(c, YH, part.at[ts, blk(x, 1 - yh)], ry.at[ts], d_yh)

    def grows(c, s, count=1):
        n = 8 * CHUNKS[c]
        return pl.ds(pl.multiple_of(128 * STARTS[c] + s * n, 8), count * n)

    def whole(c, s, count=1):
        return gath.at[:, grows(c, s, count), :]

    def pair(c, zz):
        if c in Z_FIRST:
            return grows(c, slot(zz, yl, core))
        return grows(c, slot(zz, 0, core), 2)

    def half(c, zz, lo):
        return gath.at[pl.ds(lo, O_LOC // 2), pair(c, zz), :]

    def task_h(c):
        cps[c, YH].wait_recv()
        base = 128 * STARTS[c] + me * (8 * CHUNKS[c])

        @functools.partial(each_tile, c)
        def _(t):
            h = (xsum(t, yh) + ry[t].astype(F32)).astype(BF)
            h = jnp.dot(h, onehot[...], preferred_element_type=F32).astype(BF)
            dst = pl.ds(pl.multiple_of(base + (t - STARTS[c]) * 8, 8), 8)
            gath[:, dst, :] = h.reshape(O_LOC, 8, NP)

        g = whole(c, me)
        go(c, AY, g, g, d_yl)
        go(c, AZP, g, g, d_zp)
        go(c, AZM, g, g, d_zm)
        go(c, AC, g, g, d_co)

    def task_b(c):
        cps[c, AY].wait_recv()
        g = whole(c, slot(z, 1 - yl, core))
        if c not in Z_FIRST:
            go(c, BZP, g, g, d_zp)
            go(c, BZM, g, g, d_zm)
        go(c, BC, g, g, d_co)

    def spread(c, zz, to_core, to_y):
        g = gath.at[:, pair(c, zz), :]
        go(c, to_core, g, g, d_co)
        if c in Z_FIRST:
            go(c, to_y, g, g, d_yl)

    def task_cp(c):
        cps[c, AZP].wait_recv()
        if c not in Z_FIRST:
            cps[c, BZP].wait_recv()
        g = half(c, zm, 0)
        go(c, CZP, g, g, d_zp)
        spread(c, zm, CCP, BYP)

    def task_cm(c):
        cps[c, AZM].wait_recv()
        if c not in Z_FIRST:
            cps[c, BZM].wait_recv()
        g = half(c, zp, O_LOC // 2)
        go(c, CZM, g, g, d_zm)
        spread(c, zp, CCM, BYM)

    def task_d(c):
        cps[c, CZP].wait_recv()
        cps[c, CZM].wait_recv()
        spread(c, z2, DC, BY2)

    def across(c, zz, arrived, to_core):
        cps[c, arrived].wait_recv()
        g = whole(c, slot(zz, 1 - yl, core))
        go(c, to_core, g, g, d_co)

    def task_yp(c):
        across(c, zm, BYP, YCP)

    def task_ym(c):
        across(c, zp, BYM, YCM)

    def task_y2(c):
        across(c, z2, BY2, YC2)

    def task_vt(_):
        vlocal().wait()

        @pl.loop(1, 16)
        def _(k):
            vcopy(k).wait()

        for c in range(len(CHUNKS)):
            n = 8 * CHUNKS[c]

            @pl.loop(0, 16)
            def _(s):
                dst = pl.ds(pl.multiple_of(128 * STARTS[c] + s * n, 8), n)
                vrows[dst, :] = vrecv[s, pl.ds(8 * STARTS[c], n), :]

        @pl.loop(0, TILES)
        def _(t):
            o = pl.multiple_of(t * 128, 128)
            vt[:, pl.ds(o, 128)] = vrows[pl.ds(o, 128), :].astype(F32).T[:A_LOC].astype(BF)

    def task_e(c):
        for k in (AC, BC, CCP, CCM, DC) + ((YCP, YCM, YC2) if c in Z_FIRST else ()):
            cps[c, k].wait_recv()
        ks = pl.ds(128 * STARTS[c], 128 * CHUNKS[c])
        lhs = vt[:, ks]
        last = c == len(CHUNKS) - 1

        @pl.loop(0, O_LOC, unroll=O_LOC)
        def _(i):
            d = jnp.dot(lhs, gath[i, ks, :], preferred_element_type=F32)
            if c > 0:
                d = d + acc[i]
            if last:
                out[i] = d.astype(BF)
            else:
                acc[i] = d

    tasks = {"M": task_m, "X": task_x, "SP": task_sp, "SM": task_sm, "Y": task_y, "H": task_h, "B": task_b,
             "YP": task_yp, "YM": task_ym, "Y2": task_y2, "CP": task_cp, "CM": task_cm, "D": task_d, "E": task_e, "VS": task_vs, "VP": task_vp, "VT": task_vt}
    for name, *where in ORDER:
        tasks[name](*where)
    for cp in sent:
        cp.wait_send()


def local(integrals, occ_coef, virt_coef, pair_index):
    nsem = NSEM * len(CHUNKS)
    vm = pl.BlockSpec(memory_space=pltpu.VMEM)
    hbm = pl.BlockSpec(memory_space=pl.ANY)
    return pl.pallas_call(
        kernel,
        out_shape=jax.ShapeDtypeStruct((O_LOC, A_LOC, NP), BF),
        in_specs=[hbm, vm, hbm, vm],
        out_specs=vm,
        scratch_shapes=[
            pltpu.VMEM((NBUF, N_MU, 8, NP), BF),
            pltpu.VMEM((8 * BLK, KROWS), BF),
            pltpu.VMEM((8 * BLK, 8 * O_LOC), BF),
            pltpu.VMEM((NP, NP), BF),
            pltpu.VMEM((TILES, 8 * BLK, NP), BF),
            pltpu.VMEM((TILES, BLK, NP), BF),
            pltpu.VMEM((TILES, BLK, NP), BF),
            pltpu.VMEM((TILES, 2 * BLK, NP), BF),
            pltpu.VMEM((TILES, 2 * BLK, NP), BF),
            pltpu.VMEM((TILES, BLK, NP), BF),
            pltpu.VMEM((O_LOC, TILES * 128, NP), BF),
            pltpu.VMEM((N_NU, 16 * A_LOC), BF),
            pltpu.VMEM((16, 8 * TILES, NP), BF),
            pltpu.VMEM((16, 8 * TILES, NP), BF),
            pltpu.VMEM((TILES * 128, NP), BF),
            pltpu.VMEM((A_LOC, TILES * 128), BF),
            pltpu.VMEM((O_LOC, A_LOC, NP), F32),
            pltpu.SemaphoreType.DMA((NBUF,)),
            pltpu.SemaphoreType.DMA,
            pltpu.SemaphoreType.DMA((16,)),
            pltpu.SemaphoreType.DMA((16,)),
            pltpu.SemaphoreType.DMA((nsem,)),
            pltpu.SemaphoreType.DMA((nsem,)),
        ],
        compiler_params=pltpu.CompilerParams(
            collective_id=0, has_side_effects=True, vmem_limit_bytes=60 * 2**20
        ),
    )(integrals, occ_coef.T, virt_coef, pair_index[None, :])


def solution(mesh):
    return jax.shard_map(
        local,
        mesh=mesh,
        in_specs=(P("row", "col", None), P("row", None), P("col", None), P()),
        out_specs=P("row", "col", None),
        check_vma=False,
    )
```

```python
import functools

import jax
import jax.numpy as jnp
from jax import lax
from jax.experimental import pallas as pl
from jax.experimental.pallas import tpu as pltpu
from jax.sharding import PartitionSpec as P

MESH = pl.DeviceIdType.MESH
BF = jnp.bfloat16
F32 = jnp.float32

N_MU = 300
N_NU = 150
O_LOC = 12
A_LOC = 144
NP = 256
TILES = 19
CHUNKS = (2, 1, 3, 4, 2, 2, 3, 2)
Z_FIRST = (1, 4, 7)
STARTS = tuple(sum(CHUNKS[:k]) for k in range(len(CHUNKS)))
BLK = O_LOC * 8
KROWS = N_MU * 8
NBUF = 3

(X1P, X1M, RAWP, RAWM, ACCP, ACCM, YH, AZP, AZM, AY, AC, BZP, BZM, BC, CZP, CZM, CCP, CCM, DC,
 BYP, BYM, BY2, YCP, YCM, YC2) = range(25)
NSEM = 25

STEPS = (
    (),
    (("X", 0), ("VS", 0),),
    (("VP", 0), ("X", 1),),
    (("SP", 0), ("SM", 0),),
    (),
    (("X", 2),),
    (("SM", 1),),
    (),
    (("Y", 0),),
    (("SP", 1),),
    (("SM", 2), ("SP", 2),),
    (),
    (("Y", 1), ("X", 3),),
    (),
    (("Y", 2),),
    (("H", 1),),
    (("H", 0), ("SP", 3), ("SM", 3), ("H", 2), ("CM", 1), ("CP", 1), ("VT", 0), ("X", 4), ("X", 5), ("B", 0),
     ("Y", 3), ("B", 2),),
    (("CM", 0), ("SP", 4), ("CP", 0), ("D", 1), ("SM", 4),),
    (("YP", 1), ("SP", 5), ("B", 1), ("SM", 5), ("CM", 2), ("CP", 2), ("H", 3), ("Y2", 1), ("X", 6), ("D", 0),
     ("Y", 4), ("E", 0), ("Y", 5), ("YM", 1), ("D", 2), ("B", 3), ("SP", 6), ("SM", 6), ("E", 1), ("X", 7),
     ("H", 4), ("H", 5), ("CP", 3), ("CM", 3), ("Y", 6), ("SP", 7), ("SM", 7), ("B", 5), ("CP", 4), ("CM", 4),
     ("Y", 7), ("H", 6), ("D", 3), ("B", 4), ("E", 2), ("CP", 5), ("YM", 4), ("E", 3), ("YP", 4), ("CM", 5),
     ("D", 4), ("H", 7), ("B", 6), ("CM", 7), ("Y2", 4), ("CP", 7), ("CP", 6), ("CM", 6), ("D", 5), ("E", 4),
     ("D", 7), ("E", 5), ("YP", 7), ("YM", 7), ("D", 6), ("Y2", 7), ("B", 7), ("E", 6), ("E", 7),),
)


def kernel(
    ints, occ_t, virt, index, out,
    ibuf, kron, pick, onehot, part, r1p, r1m, r2p, r2m, ry, gath, vraw, vblk, vrecv, vrows, vt, acc,
    isem, vload, vsend, vrecv_sem, send, recv,
):
    row = lax.axis_index("row")
    col = lax.axis_index("col")
    yh, x = row // 4, row % 4
    z, yl, core = col // 4, (col // 2) % 2, col % 2
    xp, xm = (x + 1) % 4, (x + 3) % 4
    x2 = (x + 2) % 4
    zp, zm, z2 = (z + 1) % 4, (z + 3) % 4, (z + 2) % 4

    def rowid(xx, yy):
        return {"row": yy * 4 + xx}

    def colid(zz, ll, cc):
        return {"col": zz * 4 + ll * 2 + cc}

    d_xp, d_xm, d_yh = rowid(xp, yh), rowid(xm, yh), rowid(x, 1 - yh)
    d_zp, d_zm = colid(zp, yl, core), colid(zm, yl, core)
    d_yl, d_co = colid(z, 1 - yl, core), colid(z, yl, 1 - core)

    def slot(zz, ll, cc):
        return cc * 8 + zz * 2 + ll

    me = slot(z, yl, core)

    barrier = pltpu.get_barrier_semaphore()
    for d in (d_xp, d_xm, d_yh):
        pl.semaphore_signal(barrier, inc=1, device_id=d, device_id_type=MESH)

    @pl.loop(1, 16)
    def _(k):
        pl.semaphore_signal(barrier, inc=1, device_id={"col": (col + k) % 16}, device_id_type=MESH)

    def icopy(t, s):
        return pltpu.make_async_copy(ints.at[:, pl.ds(pl.multiple_of(t * 8, 8), 8), :], ibuf.at[s], isem.at[s])

    def icopy_last(s):
        return pltpu.make_async_copy(
            ints.at[:, pl.ds(8 * (TILES - 1), 6), :], ibuf.at[s, :, pl.ds(0, 6), :], isem.at[s]
        )

    for t in range(NBUF):
        icopy(t, t).start()

    def vfetch():
        return pltpu.make_async_copy(virt, vraw, vload)

    vfetch().start()

    def iota(shape, axis):
        return lax.broadcasted_iota(jnp.int32, shape, axis)

    for b in range(8):
        first = ((b % 2) * 4 + b // 2) * O_LOC
        mine = iota((BLK, 8 * O_LOC), 1) == first + (iota((BLK, 8 * O_LOC), 0) >> 3)
        pick[b * BLK : (b + 1) * BLK, :] = jnp.where(mine, 1.0, 0.0).astype(BF)
    same = ((iota((8, NP), 0) & 7) == (iota((8, NP), 1) & 7))[None]
    for j in range(0, N_MU, 32):
        n = min(32, N_MU - j)
        stretch = jnp.where(iota((n, 8 * n), 0) == (iota((n, 8 * n), 1) >> 3), 1.0, 0.0).astype(BF)
        wide = jnp.dot(occ_t[:, j : j + n], stretch, preferred_element_type=F32).astype(BF)
        wide = jnp.dot(pick[...], wide, preferred_element_type=F32).reshape(8 * O_LOC, 8, 8 * n)
        wide = jnp.where(same[:, :, : 8 * n], wide, 0.0).astype(BF)
        kron[:, 8 * j : 8 * (j + n)] = wide.reshape(8 * BLK, 8 * n)

    onehot[...] = jnp.where(iota((NP, NP), 0) == index[...], 1.0, 0.0).astype(BF)

    pl.semaphore_wait(barrier, 18)

    sent = []

    def remote(src, dst, c, k, dev):
        return pltpu.make_async_remote_copy(
            src_ref=src, dst_ref=dst, send_sem=send.at[c * NSEM + k], recv_sem=recv.at[c * NSEM + k],
            device_id=dev, device_id_type=MESH,
        )

    def go(c, k, src, dst, dev):
        remote(src, dst, c, k, dev).start()
        sent.append((c, k))

    def like(c, k):
        n = CHUNKS[c]
        rows = 8 * n * (2 if k in (CZP, CZM, CCP, CCM, DC) and c not in Z_FIRST else 1)
        if k <= YH:
            ref = part.at[pl.ds(0, n), pl.ds(0, BLK), :]
        elif k in (CZP, CZM):
            ref = gath.at[pl.ds(0, O_LOC // 2), pl.ds(0, rows), :]
        else:
            ref = gath.at[:, pl.ds(0, rows), :]
        return remote(ref, ref, c, k, d_co)

    def arrived(c, k):
        like(c, k).wait_recv()

    def vcopy(k):
        to = (col + k) % 16
        to_slot = slot(to // 4, (to // 2) % 2, to % 2)
        return pltpu.make_async_remote_copy(
            src_ref=vblk.at[to_slot], dst_ref=vrecv.at[me], send_sem=vsend.at[k], recv_sem=vrecv_sem.at[k],
            device_id={"col": to}, device_id_type=MESH,
        )

    def vlocal():
        return pltpu.make_async_copy(vblk.at[me], vrecv.at[me], vsend.at[0])

    def task_vs(_):
        vfetch().wait()
        for k in range(16):
            s = slot(k // 4, (k // 2) % 2, k % 2)
            vblk[s, N_NU - 6 : 8 * TILES, :] = jnp.zeros((8, NP), BF)
            vblk[s, 0:N_NU, 0:A_LOC] = vraw[:, k * A_LOC : (k + 1) * A_LOC]

    def task_vp(_):
        vlocal().start()

        @pl.loop(1, 16)
        def _(k):
            vcopy(k).start()

    def tiles(c):
        return pl.ds(STARTS[c], CHUNKS[c])

    def blk(xx, yy):
        return pl.ds(pl.multiple_of(xx * (2 * BLK) + yy * BLK, BLK), BLK)

    def product(t):
        s = t % NBUF

        @pl.when(t < TILES - 1)
        def _():
            icopy(t, s).wait()

        @pl.when(t == TILES - 1)
        def _():
            icopy_last(s).wait()

        rhs = ibuf[s].reshape(KROWS, NP)
        part[t] = jnp.dot(kron[...], rhs, preferred_element_type=F32).astype(BF)

        @pl.when(t + NBUF < TILES - 1)
        def _():
            icopy(t + NBUF, s).start()

        @pl.when(t + NBUF == TILES - 1)
        def _():
            icopy_last(s).start()

    def task_x(c):
        ts = tiles(c)
        go(c, X1P, part.at[ts, blk(x2, 0)], r1p.at[ts], d_xp)
        go(c, X1M, part.at[ts, blk(x2, 1)], r1m.at[ts], d_xm)
        go(c, RAWP, part.at[ts, blk(xp, 1)], r2p.at[ts, pl.ds(BLK, BLK)], d_xp)
        go(c, RAWM, part.at[ts, blk(xm, 0)], r2m.at[ts, pl.ds(0, BLK)], d_xm)

    def each_tile(c, body):
        pl.loop(STARTS[c], STARTS[c] + CHUNKS[c])(body)

    def task_sp(c):
        ts = tiles(c)
        arrived(c, X1P)

        @functools.partial(each_tile, c)
        def _(t):
            b = blk(xp, 0)
            part[t, b, :] = (part[t, b, :].astype(F32) + r1p[t].astype(F32)).astype(BF)

        go(c, ACCP, part.at[ts, blk(xp, 0)], r2p.at[ts, pl.ds(0, BLK)], d_xp)

    def task_sm(c):
        ts = tiles(c)
        arrived(c, X1M)

        @functools.partial(each_tile, c)
        def _(t):
            b = blk(xm, 1)
            part[t, b, :] = (part[t, b, :].astype(F32) + r1m[t].astype(F32)).astype(BF)

        go(c, ACCM, part.at[ts, blk(xm, 1)], r2m.at[ts, pl.ds(BLK, BLK)], d_xm)

    def xsum(t, yy):
        side = pl.ds(pl.multiple_of(yy * BLK, BLK), BLK)
        return part[t, blk(x, yy), :].astype(F32) + r2p[t, side, :].astype(F32) + r2m[t, side, :].astype(F32)

    def task_y(c):
        ts = tiles(c)
        for k in (RAWP, RAWM, ACCP, ACCM):
            arrived(c, k)

        @functools.partial(each_tile, c)
        def _(t):
            part[t, blk(x, 1 - yh), :] = xsum(t, 1 - yh).astype(BF)

        go(c, YH, part.at[ts, blk(x, 1 - yh)], ry.at[ts], d_yh)

    def grows(c, s, count=1):
        n = 8 * CHUNKS[c]
        return pl.ds(pl.multiple_of(128 * STARTS[c] + s * n, 8), count * n)

    def whole(c, s, count=1):
        return gath.at[:, grows(c, s, count), :]

    def pair(c, zz):
        if c in Z_FIRST:
            return grows(c, slot(zz, yl, core))
        return grows(c, slot(zz, 0, core), 2)

    def half(c, zz, lo):
        return gath.at[pl.ds(lo, O_LOC // 2), pair(c, zz), :]

    def task_h(c):
        arrived(c, YH)
        base = 128 * STARTS[c] + me * (8 * CHUNKS[c])

        @functools.partial(each_tile, c)
        def _(t):
            h = (xsum(t, yh) + ry[t].astype(F32)).astype(BF)
            h = jnp.dot(h, onehot[...], preferred_element_type=F32).astype(BF)
            dst = pl.ds(pl.multiple_of(base + (t - STARTS[c]) * 8, 8), 8)
            gath[:, dst, :] = h.reshape(O_LOC, 8, NP)

        g = whole(c, me)
        go(c, AY, g, g, d_yl)
        go(c, AZP, g, g, d_zp)
        go(c, AZM, g, g, d_zm)
        go(c, AC, g, g, d_co)

    def task_b(c):
        arrived(c, AY)
        g = whole(c, slot(z, 1 - yl, core))
        if c not in Z_FIRST:
            go(c, BZP, g, g, d_zp)
            go(c, BZM, g, g, d_zm)
        go(c, BC, g, g, d_co)

    def spread(c, zz, to_core, to_y):
        g = gath.at[:, pair(c, zz), :]
        go(c, to_core, g, g, d_co)
        if c in Z_FIRST:
            go(c, to_y, g, g, d_yl)

    def task_cp(c):
        arrived(c, AZP)
        if c not in Z_FIRST:
            arrived(c, BZP)
        g = half(c, zm, 0)
        go(c, CZP, g, g, d_zp)
        spread(c, zm, CCP, BYP)

    def task_cm(c):
        arrived(c, AZM)
        if c not in Z_FIRST:
            arrived(c, BZM)
        g = half(c, zp, O_LOC // 2)
        go(c, CZM, g, g, d_zm)
        spread(c, zp, CCM, BYM)

    def task_d(c):
        arrived(c, CZP)
        arrived(c, CZM)
        spread(c, z2, DC, BY2)

    def across(c, zz, landed, to_core):
        arrived(c, landed)
        g = whole(c, slot(zz, 1 - yl, core))
        go(c, to_core, g, g, d_co)

    def task_yp(c):
        across(c, zm, BYP, YCP)

    def task_ym(c):
        across(c, zp, BYM, YCM)

    def task_y2(c):
        across(c, z2, BY2, YC2)

    def task_vt(_):
        vlocal().wait()

        @pl.loop(1, 16)
        def _(k):
            vcopy(k).wait()

        for c in range(len(CHUNKS)):
            n = 8 * CHUNKS[c]

            @pl.loop(0, 16)
            def _(s):
                dst = pl.ds(pl.multiple_of(128 * STARTS[c] + s * n, 8), n)
                vrows[dst, :] = vrecv[s, pl.ds(8 * STARTS[c], n), :]

        @pl.loop(0, TILES)
        def _(t):
            o = pl.multiple_of(t * 128, 128)
            vt[:, pl.ds(o, 128)] = vrows[pl.ds(o, 128), :].astype(F32).T[:A_LOC].astype(BF)

    def task_e(c):
        for k in (AC, BC, CCP, CCM, DC) + ((YCP, YCM, YC2) if c in Z_FIRST else ()):
            arrived(c, k)
        ks = pl.ds(128 * STARTS[c], 128 * CHUNKS[c])
        lhs = vt[:, ks]
        last = c == len(CHUNKS) - 1

        @pl.loop(0, O_LOC, unroll=O_LOC)
        def _(i):
            d = jnp.dot(lhs, gath[i, ks, :], preferred_element_type=F32)
            if c > 0:
                d = d + acc[i]
            if last:
                out[i] = d.astype(BF)
            else:
                acc[i] = d

    tasks = {"X": task_x, "SP": task_sp, "SM": task_sm, "Y": task_y, "H": task_h, "B": task_b,
             "CP": task_cp, "CM": task_cm, "D": task_d, "YP": task_yp, "YM": task_ym, "Y2": task_y2,
             "E": task_e, "VS": task_vs, "VP": task_vp, "VT": task_vt}

    def steps(k):
        for name, c in STEPS[k]:
            tasks[name](c)

    @pl.loop(0, TILES)
    def _(t):
        product(t)
        for k in range(TILES - 1):
            if STEPS[k]:
                pl.when(t == k)(functools.partial(steps, k))

    steps(TILES - 1)
    for c, k in sent:
        like(c, k).wait_send()


def local(integrals, occ_coef, virt_coef, pair_index):
    nsem = NSEM * len(CHUNKS)
    vm = pl.BlockSpec(memory_space=pltpu.VMEM)
    hbm = pl.BlockSpec(memory_space=pl.ANY)
    return pl.pallas_call(
        kernel,
        out_shape=pltpu.VMEM((O_LOC, A_LOC, NP), BF),
        in_specs=[hbm, vm, hbm, vm],
        out_specs=vm,
        scratch_shapes=[
            pltpu.VMEM((NBUF, N_MU, 8, NP), BF),
            pltpu.VMEM((8 * BLK, KROWS), BF),
            pltpu.VMEM((8 * BLK, 8 * O_LOC), BF),
            pltpu.VMEM((NP, NP), BF),
            pltpu.VMEM((TILES, 8 * BLK, NP), BF),
            pltpu.VMEM((TILES, BLK, NP), BF),
            pltpu.VMEM((TILES, BLK, NP), BF),
            pltpu.VMEM((TILES, 2 * BLK, NP), BF),
            pltpu.VMEM((TILES, 2 * BLK, NP), BF),
            pltpu.VMEM((TILES, BLK, NP), BF),
            pltpu.VMEM((O_LOC, TILES * 128, NP), BF),
            pltpu.VMEM((N_NU, 16 * A_LOC), BF),
            pltpu.VMEM((16, 8 * TILES, NP), BF),
            pltpu.VMEM((16, 8 * TILES, NP), BF),
            pltpu.VMEM((TILES * 128, NP), BF),
            pltpu.VMEM((A_LOC, TILES * 128), BF),
            pltpu.VMEM((O_LOC, A_LOC, NP), F32),
            pltpu.SemaphoreType.DMA((NBUF,)),
            pltpu.SemaphoreType.DMA,
            pltpu.SemaphoreType.DMA((16,)),
            pltpu.SemaphoreType.DMA((16,)),
            pltpu.SemaphoreType.DMA((nsem,)),
            pltpu.SemaphoreType.DMA((nsem,)),
        ],
        compiler_params=pltpu.CompilerParams(
            collective_id=0, has_side_effects=True, vmem_limit_bytes=60 * 2**20
        ),
    )(integrals, occ_coef.T, virt_coef, pair_index[None, :])


def solution(mesh):
    return jax.shard_map(
        local,
        mesh=mesh,
        in_specs=(P("row", "col", None), P("row", None), P("col", None), P()),
        out_specs=P("row", "col", None),
        check_vma=False,
    )
```
